32 devices in a mesh: wide: 8 (over y, x, core), narrow: 4 (over z).
Axes of the slice: x: 2, y: 2, z: 4, core: 2. Of those that a mesh axis runs over, the one named last changes fastest.
Arguments:
- student_feats: bfloat16 [64, 512], P(('wide', 'narrow')), may hold values from -8 to 8
- teacher_feats: bfloat16 [64, 512], P(('wide', 'narrow')), may hold values from -8 to 8
- prototypes: bfloat16 [16384, 512], P(('wide', 'narrow')), may hold values from -8 to 8
Outputs:
- student_grad: float32 [64, 512], P(('wide', 'narrow'))
- proto_grad: float32 [16384, 512], P(('wide', 'narrow'))
The draws below stay inside these ranges and needn't reach their ends.
All inputs are finite; a program needn't handle non-finite values.
Results may differ from the reference program's by a relative error of at most 0.0006.
The reference program's roundings to bfloat16 on the way (of `student_hat`, `teacher_hat`, `proto_hat` and `grad_logits`) count: a program that leaves them out, or rounds other values in their place, can miss the bound.
Values may be sent and summed in bfloat16 or wider, within the bound.
No kernel may reach another device: no remote copies, remote signals or barrier semaphores. Data moves between devices by JAX's collectives and lax.ppermute only.
A program may use at most 64 MiB of HBM per device.

```python
import math
import jax
import jax.numpy as jnp
from jax import lax

D = 512
PROTOS = 16384
ROWS = 64
SINK_ITERS = 3


cluster_count = 16


def cluster_centers(key):
    return jax.random.normal(jax.random.fold_in(key, 7), (cluster_count, D), jnp.float32) / jnp.sqrt(jnp.float32(D))


def proto_rows(key, ident):
    centers = cluster_centers(key)
    proto_key = jax.random.fold_in(key, 3)

    def single(index):
        own_key = jax.random.fold_in(proto_key, index)
        first = jax.random.randint(jax.random.fold_in(own_key, 1), (), 0, cluster_count)
        second = jax.random.randint(jax.random.fold_in(own_key, 2), (), 0, cluster_count)
        member = jnp.minimum(first, second)
        weight = jax.random.uniform(jax.random.fold_in(own_key, 4), (), jnp.float32, 0.3, 1.0)
        noise = jax.random.normal(jax.random.fold_in(own_key, 5), (D,), jnp.float32) / jnp.sqrt(jnp.float32(D))
        return weight * centers[member] + 0.8 * noise
    return jax.vmap(single)(ident)


def features(key, salt_value):
    centers = cluster_centers(key)
    chosen_ids = jax.random.randint(jax.random.fold_in(key, 11), (ROWS,), 0, PROTOS)
    first = jax.random.randint(jax.random.fold_in(key, 12), (ROWS,), 0, cluster_count)
    second = jax.random.randint(jax.random.fold_in(key, 13), (ROWS,), 0, cluster_count)
    row_cluster = jnp.maximum(first, second)
    chosen = proto_rows(key, chosen_ids)
    center_part = centers[row_cluster]
    along = jax.random.uniform(jax.random.fold_in(key, salt_value), (ROWS, 1), jnp.float32, 0.3, 1.5)
    toward = jax.random.uniform(jax.random.fold_in(key, salt_value + 3), (ROWS, 1), jnp.float32, 0.0, 1.0)
    spread = jnp.exp(jax.random.uniform(jax.random.fold_in(key, salt_value + 4), (ROWS, 1), jnp.float32, math.log(0.1), 0.0))
    jitter = jax.random.normal(jax.random.fold_in(key, salt_value + 1), (ROWS, D), jnp.float32) / jnp.sqrt(jnp.float32(D))
    mixed = along * center_part + toward * chosen + spread * jitter
    return jnp.clip(mixed, -8.0, 8.0).astype(jnp.bfloat16)


def draw_student_feats(key, part):
    return features(key, 21)


def draw_teacher_feats(key, part):
    return features(key, 31)


def draw_prototypes(key, part):
    protos = proto_rows(key, jnp.arange(PROTOS, dtype=jnp.int32))
    return jnp.clip(protos, -8.0, 8.0).astype(jnp.bfloat16)


def setup_inputs(seed: int = 0) -> dict:
    splits = jax.random.split(jax.random.key(seed), 4)
    student_feats = draw_student_feats(jax.random.fold_in(splits[3], 71), 0)
    teacher_feats = draw_teacher_feats(jax.random.fold_in(splits[3], 71), 0)
    prototypes = draw_prototypes(jax.random.fold_in(splits[3], 71), 0)
    return dict(student_feats=student_feats, teacher_feats=teacher_feats, prototypes=prototypes)


epsilon = 1e-06
teacher_temp = 0.07
student_temp = 0.1
loss_scale = 1.0

def unit_rows(values):
    widened = values.astype(jnp.float32)
    inverse = lax.rsqrt(lax.optimization_barrier(jnp.sum(widened * widened, axis=1, keepdims=True)) + epsilon)
    return (widened * inverse, inverse)

def reference(student_feats, teacher_feats, prototypes):
    student_unit, student_inv = unit_rows(student_feats)
    teacher_unit = unit_rows(teacher_feats)[0]
    proto_unit, proto_inv = unit_rows(prototypes)
    student_hat = student_unit.astype(jnp.bfloat16)
    teacher_hat = teacher_unit.astype(jnp.bfloat16)
    proto_hat = proto_unit.astype(jnp.bfloat16)
    logits = jnp.dot(student_hat, proto_hat.T, preferred_element_type=jnp.float32)
    teacher_logits = jnp.dot(teacher_hat, proto_hat.T, preferred_element_type=jnp.float32)
    exp_teacher = jnp.exp(teacher_logits / teacher_temp)
    row_scale = jnp.ones((ROWS,), jnp.float32)
    col_scale = jnp.ones((PROTOS,), jnp.float32)
    for sweep in range(SINK_ITERS):
        col_scale = 1.0 / lax.optimization_barrier(jnp.sum(exp_teacher * row_scale[:, None], axis=0))
        row_scale = 1.0 / lax.optimization_barrier(jnp.sum(exp_teacher * col_scale[None, :], axis=1))
    target = row_scale[:, None] * exp_teacher * col_scale[None, :]
    exp_student = jnp.exp(logits / student_temp)
    student_prob = exp_student / lax.optimization_barrier(jnp.sum(exp_student, axis=1, keepdims=True))
    grad_logits = (loss_scale * (student_prob - target) / student_temp).astype(jnp.bfloat16)
    proto_step = jnp.dot(grad_logits.T, student_hat, preferred_element_type=jnp.float32)
    proto_grad = (proto_step - proto_unit * lax.optimization_barrier(jnp.sum(proto_unit * proto_step, axis=1, keepdims=True))) * proto_inv
    row_step = jnp.dot(grad_logits, proto_hat, preferred_element_type=jnp.float32)
    student_grad = (row_step - student_unit * lax.optimization_barrier(jnp.sum(student_unit * row_step, axis=1, keepdims=True))) * student_inv
    return (student_grad, proto_grad)
```

```python
import jax
import jax.numpy as jnp
from jax import lax
from jax.sharding import PartitionSpec as P

SINK_ITERS = 3
AXES = ("wide", "narrow")

epsilon = 1e-06
teacher_temp = 0.07
student_temp = 0.1
loss_scale = 1.0


def unit_rows(values):
    widened = values.astype(jnp.float32)
    inverse = lax.rsqrt(jnp.sum(widened * widened, axis=1, keepdims=True) + epsilon)
    return (widened * inverse, inverse)


def on_device(devices, student_feats, teacher_feats, prototypes):
    def to_all(block):
        spread = jnp.broadcast_to(block[None], (devices,) + block.shape)
        return lax.all_to_all(spread, AXES, 0, 0, tiled=True)

    def total(partial_value):
        return jnp.sum(to_all(partial_value), axis=0)

    own_rows, width = student_feats.shape
    rows = devices * own_rows
    student_unit, student_inv = unit_rows(student_feats)
    teacher_unit = unit_rows(teacher_feats)[0]
    paired = jnp.stack([student_unit, teacher_unit]).astype(jnp.bfloat16)
    gathered = jnp.swapaxes(to_all(paired), 0, 1).reshape(2, rows, width)
    proto_unit, proto_inv = unit_rows(prototypes)
    proto_hat = proto_unit.astype(jnp.bfloat16)
    logits = jnp.einsum("srd,pd->srp", gathered, proto_hat, preferred_element_type=jnp.float32)
    exp_student = jnp.exp(logits[0] / student_temp)
    exp_teacher = jnp.exp(logits[1] / teacher_temp)
    student_part = jnp.sum(exp_student, axis=1)
    col_scale = 1.0 / jnp.sum(exp_teacher, axis=0)
    for sweep in range(SINK_ITERS - 1):
        row_scale = 1.0 / total(jnp.sum(exp_teacher * col_scale[None, :], axis=1))
        col_scale = 1.0 / jnp.sum(exp_teacher * row_scale[:, None], axis=0)
    teacher_part = jnp.sum(exp_teacher * col_scale[None, :], axis=1)
    totals = total(jnp.stack([teacher_part, student_part]))
    row_scale = 1.0 / totals[0]
    target = row_scale[:, None] * exp_teacher * col_scale[None, :]
    student_prob = exp_student / totals[1][:, None]
    grad_logits = (loss_scale * (student_prob - target) / student_temp).astype(jnp.bfloat16)
    row_part = jnp.einsum("bp,pd->bd", grad_logits, proto_hat, preferred_element_type=jnp.float32)
    row_parts = lax.all_to_all(row_part.reshape(devices, own_rows, width), AXES, 0, 0, tiled=True)
    proto_step = jnp.einsum(
        "bp,bd->pd", grad_logits, gathered[0], preferred_element_type=jnp.float32
    )
    proto_grad = (
        proto_step - proto_unit * jnp.sum(proto_unit * proto_step, axis=1, keepdims=True)
    ) * proto_inv
    row_step = jnp.sum(row_parts, axis=0)
    student_grad = (
        row_step - student_unit * jnp.sum(student_unit * row_step, axis=1, keepdims=True)
    ) * student_inv
    return (student_grad, proto_grad)


def solution(mesh):
    placed = P(AXES, None)
    devices = 1
    for axis in AXES:
        devices *= mesh.shape[axis]

    def body(*args):
        return on_device(devices, *args)

    return jax.shard_map(
        body,
        mesh=mesh,
        in_specs=(placed, placed, placed),
        out_specs=(placed, placed),
        check_vma=False,
    )
```

```python
import functools
import math

import jax
import jax.numpy as jnp
from jax import lax
from jax.experimental import pallas as pl
from jax.experimental.pallas import tpu as pltpu
from jax.sharding import PartitionSpec as P

SINK_ITERS = 3
AXES = ("wide", "narrow")
LANES = 128
MIB = 2**20

epsilon = 1e-06
teacher_temp = 0.07
student_temp = 0.1
loss_scale = 1.0

F32 = jnp.float32
BF16 = jnp.bfloat16


def unit_rows(values):
    widened = values.astype(F32)
    inverse = lax.rsqrt(jnp.sum(widened * widened, axis=1, keepdims=True) + epsilon)
    return (widened * inverse, inverse)


def dot(lhs, rhs, lhs_dim, rhs_dim):
    return lax.dot_general(
        lhs, rhs, (((lhs_dim,), (rhs_dim,)), ((), ())), preferred_element_type=F32
    )


def hat_kernel(student_ref, teacher_ref, out_ref):
    devices, both, width = out_ref.shape
    rows = both // 2
    hats = jnp.concatenate(
        [unit_rows(student_ref[...])[0], unit_rows(teacher_ref[...])[0]], axis=0
    ).astype(BF16)
    out_ref[...] = jnp.broadcast_to(hats[None], out_ref.shape)


def first_kernel(hats_ref, protos_ref, teacher_ref, student_ref, hat_ref, part_ref):
    proto_hat = unit_rows(protos_ref[...])[0].astype(BF16)
    hat_ref[...] = proto_hat
    exp_student = jnp.exp(dot(proto_hat, hats_ref[0], 1, 1) / student_temp)
    exp_teacher = jnp.exp(dot(proto_hat, hats_ref[1], 1, 1) / teacher_temp)
    student_ref[...] = exp_student
    teacher_ref[...] = exp_teacher
    col_scale = 1.0 / jnp.sum(exp_teacher, axis=1, keepdims=True)
    part = jnp.concatenate(
        [
            jnp.sum(exp_teacher * col_scale, axis=0, keepdims=True),
            jnp.sum(exp_student, axis=0, keepdims=True),
        ],
        axis=1,
    )
    part_ref[...] = jnp.broadcast_to(part[None], part_ref.shape)


def sweep_kernel(mass_ref, teacher_ref, part_ref):
    rows = teacher_ref.shape[1]
    exp_teacher = teacher_ref[...]
    row_scale = 1.0 / jnp.sum(mass_ref[...], axis=0)[:, :rows]
    col_scale = 1.0 / jnp.sum(exp_teacher * row_scale, axis=1, keepdims=True)
    part = jnp.sum(exp_teacher * col_scale, axis=0, keepdims=True)
    part_ref[...] = jnp.broadcast_to(part[None], part_ref.shape)


def last_sweep_kernel(mass_ref, teacher_ref, part_ref, col_ref):
    rows = teacher_ref.shape[1]
    exp_teacher = teacher_ref[...]
    row_scale = 1.0 / jnp.sum(mass_ref[...], axis=0)[:, :rows]
    col_scale = 1.0 / jnp.sum(exp_teacher * row_scale, axis=1, keepdims=True)
    col_ref[...] = col_scale
    part = jnp.sum(exp_teacher * col_scale, axis=0, keepdims=True)
    part_ref[...] = jnp.broadcast_to(part[None], part_ref.shape)


def grad_kernel(
    first_ref, mass_ref, teacher_ref, student_ref, col_ref, hat_ref, logit_ref, out_ref, step_ref
):
    rows = teacher_ref.shape[1]
    devices = first_ref.shape[0]
    own, width = rows // devices, hat_ref.shape[1]
    student_total = jnp.sum(first_ref[...], axis=0)[:, rows:]
    row_scale = 1.0 / jnp.sum(mass_ref[...], axis=0)
    target = row_scale * teacher_ref[...] * col_ref[...]
    student_prob = student_ref[...] / student_total
    grad_logits = (loss_scale * (student_prob - target) / student_temp).astype(BF16)
    logit_ref[...] = grad_logits
    row_part = dot(grad_logits, hat_ref[...], 0, 0)
    blocks = width // LANES
    for block in range(blocks):
        step_ref[block * rows : (block + 1) * rows, :] = row_part[
            :, block * LANES : (block + 1) * LANES
        ]
    for row in range(own):
        for block in range(blocks):
            out_ref[:, row * blocks + block, :] = step_ref[
                pl.ds(block * rows + row, devices, stride=own), :
            ]


def proto_kernel(logit_ref, hats_ref, protos_ref, out_ref):
    proto_unit, proto_inv = unit_rows(protos_ref[...])
    proto_step = dot(logit_ref[...], hats_ref[0], 1, 0)
    out_ref[...] = (
        proto_step - proto_unit * jnp.sum(proto_unit * proto_step, axis=1, keepdims=True)
    ) * proto_inv


def row_kernel(parts_ref, student_ref, out_ref, step_ref):
    own, width = student_ref.shape
    blocks = width // LANES
    summed = jnp.sum(parts_ref[...], axis=0)
    for row in range(own):
        for block in range(blocks):
            index = row * blocks + block
            step_ref[row : row + 1, block * LANES : (block + 1) * LANES] = summed[index : index + 1]
    row_step = step_ref[...]
    student_unit, student_inv = unit_rows(student_ref[...])
    out_ref[...] = (
        row_step - student_unit * jnp.sum(student_unit * row_step, axis=1, keepdims=True)
    ) * student_inv


def padded_bytes(shape, dtype):
    lanes = -(-shape[-1] // LANES) * LANES
    sublanes = -(-shape[-2] // 8) * 8
    return math.prod(shape[:-2]) * sublanes * lanes * jnp.dtype(dtype).itemsize


def call(kernel, outs, *args, scratch=(), flops=1000):
    vmem = pl.BlockSpec(memory_space=pltpu.VMEM)
    single = not isinstance(outs, (tuple, list))
    shapes = [outs] if single else list(outs)
    sizes = [(shape, dtype) for shape, dtype in shapes] + [(a.shape, a.dtype) for a in args]
    held = sum(padded_bytes(shape, dtype) for shape, dtype in sizes)
    result = pl.pallas_call(
        kernel,
        compiler_params=pltpu.CompilerParams(vmem_limit_bytes=2 * held + 4 * MIB),
        out_shape=[jax.ShapeDtypeStruct(shape, dtype) for shape, dtype in shapes],
        in_specs=[vmem] * len(args),
        out_specs=[vmem] * len(shapes),
        scratch_shapes=list(scratch),
        cost_estimate=pl.CostEstimate(flops=flops, bytes_accessed=0, transcendentals=0),
    )(*args)
    return result[0] if single else result


def on_device(devices, student_feats, teacher_feats, prototypes):
    def exchange(parts):
        return lax.all_to_all(parts, AXES, 0, 0, tiled=True)

    own, width = student_feats.shape
    protos = prototypes.shape[0]
    rows = devices * own
    tiles = own * width // LANES
    hats = exchange(call(hat_kernel, [((devices, 2 * own, width), BF16)], student_feats, teacher_feats)[0])
    hats = hats.reshape(devices, 2, own, width).swapaxes(0, 1).reshape(2, rows, width)
    exp_teacher, exp_student, proto_hat, part = call(
        first_kernel,
        [
            ((protos, rows), F32),
            ((protos, rows), F32),
            ((protos, width), BF16),
            ((devices, 1, 2 * rows), F32),
        ],
        hats,
        prototypes,
    )
    first = mass = exchange(part)
    for sweep in range(SINK_ITERS - 2):
        mass = exchange(call(sweep_kernel, [((devices, 1, rows), F32)], mass, exp_teacher)[0])
    part, col_scale = call(
        last_sweep_kernel, [((devices, 1, rows), F32), ((protos, 1), F32)], mass, exp_teacher
    )
    mass = exchange(part)
    grad_logits, parts = call(
        grad_kernel,
        [((protos, rows), BF16), ((devices, tiles, LANES), F32)],
        first,
        mass,
        exp_teacher,
        exp_student,
        col_scale,
        proto_hat,
        scratch=[pltpu.VMEM((rows * width // LANES, LANES), F32)],
    )
    parts = exchange(parts)
    proto_grad = call(
        proto_kernel, [((protos, width), F32)], grad_logits, hats, prototypes, flops=10**9
    )[0]
    student_grad = call(
        row_kernel,
        [((own, width), F32)],
        parts,
        student_feats,
        scratch=[pltpu.VMEM((own, width), F32)],
    )[0]
    return (student_grad, proto_grad)


def solution(mesh):
    placed = P(AXES, None)
    devices = 1
    for axis in AXES:
        devices *= mesh.shape[axis]
    return jax.shard_map(
        functools.partial(on_device, devices),
        mesh=mesh,
        in_specs=(placed, placed, placed),
        out_specs=(placed, placed),
        check_vma=False,
    )
```

```python
import functools
import math

import jax
import jax.numpy as jnp
from jax import lax
from jax.experimental import pallas as pl
from jax.experimental.pallas import tpu as pltpu
from jax.sharding import PartitionSpec as P

SINK_ITERS = 3
AXES = ("wide", "narrow")
LANES = 128
MIB = 2**20
CHUNKS = 4

epsilon = 1e-06
teacher_temp = 0.07
student_temp = 0.1
loss_scale = 1.0

F32 = jnp.float32
BF16 = jnp.bfloat16


def unit_rows(values):
    widened = values.astype(F32)
    inverse = lax.rsqrt(jnp.sum(widened * widened, axis=1, keepdims=True) + epsilon)
    return (widened * inverse, inverse)


def narrow(values):
    scaled = values * 65537.0
    return scaled - (scaled - values)


def unit_rows_close(values):
    widened = values.astype(F32)
    squares = widened * widened
    step = 2.0 * jnp.sum(squares, axis=1, keepdims=True)
    high = (squares + step) - step
    low = jnp.sum(squares - high, axis=1, keepdims=True) + epsilon
    high = jnp.sum(high, axis=1, keepdims=True)
    total = high + low
    rest = (high - total) + low
    inverse = lax.rsqrt(total)
    head = narrow(inverse)
    tail = inverse - head
    square = head * head
    total_head = narrow(total)
    total_tail = total - total_head
    total_mid = narrow(total_tail)
    miss = (1.0 - total_head * square) - total_mid * square
    miss = miss - (total_tail - total_mid) * square
    miss = miss - total * (2.0 * head * tail)
    miss = miss - (total * tail * tail + rest * square)
    inverse = inverse + 0.5 * inverse * miss
    return (widened * inverse, inverse)


def dot(lhs, rhs, lhs_dim, rhs_dim):
    return lax.dot_general(
        lhs, rhs, (((lhs_dim,), (rhs_dim,)), ((), ())), preferred_element_type=F32
    )


def hat_kernel(student_ref, teacher_ref, out_ref, held_ref, sems):
    copies = [
        pltpu.make_async_copy(source, held_ref.at[index], sems.at[index])
        for index, source in enumerate((student_ref, teacher_ref))
    ]
    for copy in copies:
        copy.start()
    for copy in copies:
        copy.wait()
    hats = jnp.concatenate([unit_rows_close(held_ref[index])[0] for index in range(2)], axis=0)
    out_ref[...] = jnp.broadcast_to(hats.astype(BF16)[None], out_ref.shape)


def first_kernel(hats_ref, protos_ref, teacher_ref, student_ref, hat_ref, inv_ref, part_ref):
    proto_unit, inv_ref[...] = unit_rows_close(protos_ref[...])
    proto_hat = proto_unit.astype(BF16)
    hat_ref[...] = proto_hat
    exp_student = jnp.exp(dot(proto_hat, hats_ref[0], 1, 1) / student_temp)
    exp_teacher = jnp.exp(dot(proto_hat, hats_ref[1], 1, 1) / teacher_temp)
    student_ref[...] = exp_student
    teacher_ref[...] = exp_teacher
    col_scale = 1.0 / jnp.sum(exp_teacher, axis=1, keepdims=True)
    part = jnp.concatenate(
        [
            jnp.sum(exp_teacher * col_scale, axis=0, keepdims=True),
            jnp.sum(exp_student, axis=0, keepdims=True),
        ],
        axis=1,
    )
    part_ref[...] = jnp.broadcast_to(part[None], part_ref.shape)


def sweep_kernel(mass_ref, teacher_ref, part_ref):
    rows = teacher_ref.shape[1]
    exp_teacher = teacher_ref[...]
    row_scale = 1.0 / jnp.sum(mass_ref[...], axis=0)[:, :rows]
    col_scale = 1.0 / jnp.sum(exp_teacher * row_scale, axis=1, keepdims=True)
    part = jnp.sum(exp_teacher * col_scale, axis=0, keepdims=True)
    part_ref[...] = jnp.broadcast_to(part[None], part_ref.shape)


def last_sweep_kernel(mass_ref, teacher_ref, part_ref, col_ref):
    rows = teacher_ref.shape[1]
    exp_teacher = teacher_ref[...]
    row_scale = 1.0 / jnp.sum(mass_ref[...], axis=0)[:, :rows]
    col_scale = 1.0 / jnp.sum(exp_teacher * row_scale, axis=1, keepdims=True)
    col_ref[...] = col_scale
    part = jnp.sum(exp_teacher * col_scale, axis=0, keepdims=True)
    part_ref[...] = jnp.broadcast_to(part[None], part_ref.shape)


def grad_kernel(
    first_ref,
    mass_ref,
    teacher_ref,
    student_ref,
    col_ref,
    hats_ref,
    hat_ref,
    protos_ref,
    inv_ref,
    out_ref,
    grad_ref,
    step_ref,
    held_ref,
    sems,
):
    protos, rows = teacher_ref.shape
    devices = first_ref.shape[0]
    own, width = rows // devices, hat_ref.shape[1]
    student_total = jnp.sum(first_ref[...], axis=0)[:, rows:]
    row_scale = 1.0 / jnp.sum(mass_ref[...], axis=0)
    target = row_scale * teacher_ref[...] * col_ref[...]
    student_prob = student_ref[...] / student_total
    grad_logits = (loss_scale * (student_prob - target) / student_temp).astype(BF16)
    copies = []
    tall = protos // CHUNKS
    for chunk in range(CHUNKS):
        part = slice(chunk * tall, (chunk + 1) * tall)
        proto_step = dot(grad_logits[part], hats_ref[0], 1, 0)
        proto_inv = inv_ref[part]
        proto_unit = protos_ref[part].astype(F32) * proto_inv
        along = jnp.sum(proto_unit * proto_step, axis=1, keepdims=True)
        held_ref[part] = (proto_step - proto_unit * along) * proto_inv
        copies.append(pltpu.make_async_copy(held_ref.at[part], grad_ref.at[part], sems.at[chunk]))
        copies[-1].start()
    row_part = dot(grad_logits, hat_ref[...], 0, 0)
    blocks = width // LANES
    for block in range(blocks):
        step_ref[block * rows : (block + 1) * rows, :] = row_part[
            :, block * LANES : (block + 1) * LANES
        ]
    for row in range(own):
        for block in range(blocks):
            out_ref[:, row * blocks + block, :] = step_ref[
                pl.ds(block * rows + row, devices, stride=own), :
            ]
    for copy in copies:
        copy.wait()


def row_kernel(parts_ref, student_ref, out_ref, step_ref):
    own, width = student_ref.shape
    blocks = width // LANES
    summed = jnp.sum(parts_ref[...], axis=0)
    for row in range(own):
        for block in range(blocks):
            index = row * blocks + block
            step_ref[row : row + 1, block * LANES : (block + 1) * LANES] = summed[index : index + 1]
    row_step = step_ref[...]
    student_unit, student_inv = unit_rows(student_ref[...])
    out_ref[...] = (
        row_step - student_unit * jnp.sum(student_unit * row_step, axis=1, keepdims=True)
    ) * student_inv


def padded_bytes(shape, dtype):
    lanes = -(-shape[-1] // LANES) * LANES
    sublanes = -(-shape[-2] // 8) * 8
    return math.prod(shape[:-2]) * sublanes * lanes * jnp.dtype(dtype).itemsize


def call(kernel, outs, *args, scratch=(), inputs=pltpu.VMEM, far=()):
    held = sum(padded_bytes(a.shape, a.dtype) for a in args)
    held += sum(padded_bytes(shape, dtype) for shape, dtype in outs)
    return pl.pallas_call(
        kernel,
        compiler_params=pltpu.CompilerParams(vmem_limit_bytes=2 * held + 4 * MIB),
        out_shape=[jax.ShapeDtypeStruct(shape, dtype) for shape, dtype in outs],
        in_specs=[pl.BlockSpec(memory_space=inputs)] * len(args),
        out_specs=[
            pl.BlockSpec(memory_space=pltpu.HBM if index in far else pltpu.VMEM)
            for index in range(len(outs))
        ],
        scratch_shapes=list(scratch),
    )(*args)


def on_device(devices, student_feats, teacher_feats, prototypes):
    def exchange(parts):
        return lax.all_to_all(parts, AXES, 0, 0, tiled=True)

    own, width = student_feats.shape
    protos = prototypes.shape[0]
    rows = devices * own
    tiles = own * width // LANES
    spread = call(
        hat_kernel,
        [((devices, 2 * own, width), BF16)],
        pltpu.with_memory_space_constraint(student_feats, pltpu.HBM),
        pltpu.with_memory_space_constraint(teacher_feats, pltpu.HBM),
        scratch=[pltpu.VMEM((2, own, width), BF16), pltpu.SemaphoreType.DMA((2,))],
        inputs=pltpu.HBM,
    )[0]
    hats = exchange(spread)
    hats = hats.reshape(devices, 2, own, width).swapaxes(0, 1).reshape(2, rows, width)
    exp_teacher, exp_student, proto_hat, proto_inv, part = call(
        first_kernel,
        [
            ((protos, rows), F32),
            ((protos, rows), F32),
            ((protos, width), BF16),
            ((protos, 1), F32),
            ((devices, 1, 2 * rows), F32),
        ],
        hats,
        prototypes,
    )
    first = mass = exchange(part)
    for sweep in range(SINK_ITERS - 2):
        mass = exchange(call(sweep_kernel, [((devices, 1, rows), F32)], mass, exp_teacher)[0])
    part, col_scale = call(
        last_sweep_kernel, [((devices, 1, rows), F32), ((protos, 1), F32)], mass, exp_teacher
    )
    mass = exchange(part)
    parts, proto_grad = call(
        grad_kernel,
        [((devices, tiles, LANES), F32), ((protos, width), F32)],
        first,
        mass,
        exp_teacher,
        exp_student,
        col_scale,
        hats,
        proto_hat,
        prototypes,
        proto_inv,
        scratch=[
            pltpu.VMEM((rows * width // LANES, LANES), F32),
            pltpu.VMEM((protos, width), F32),
            pltpu.SemaphoreType.DMA((CHUNKS,)),
        ],
        far=(1,),
    )
    student_grad = call(
        row_kernel,
        [((own, width), F32)],
        exchange(parts),
        student_feats,
        scratch=[pltpu.VMEM((own, width), F32)],
    )[0]
    return (student_grad, proto_grad)


def solution(mesh):
    placed = P(AXES, None)
    devices = 1
    for axis in AXES:
        devices *= mesh.shape[axis]
    return jax.shard_map(
        functools.partial(on_device, devices),
        mesh=mesh,
        in_specs=(placed, placed, placed),
        out_specs=(placed, placed),
        check_vma=False,
    )
```
